32 devices in a mesh: wave: 16 (over z, x, core), lev: 2 (over y).
Axes of the slice: x: 2, y: 2, z: 4, core: 2. Of those that a mesh axis runs over, the one named last changes fastest.
Arguments:
- spin_tendency: bfloat16 [32, 2, 136, 768], P('wave', None, 'lev'), may hold values from -6 to 6
- spreading_source: bfloat16 [32, 2, 136, 768], P('wave', None, 'lev'), may hold values from -6 to 6
- heat_source: bfloat16 [32, 2, 136, 768], P('wave', None, 'lev'), may hold values from -6 to 6
- helmholtz_inverses: bfloat16 [2, 384, 136, 136], P('lev', 'wave'), may hold values from -0.5 to 0.5
- heat_spreading_coupler: bfloat16 [136, 136], replicated, may hold values from -0.5 to 0.5
- smoothing_strengths: float32 [136], replicated, may hold values from 0.5 to 30
- azimuthal_order_list: int32 [32], P('wave'), may hold values from 0 to 767
Outputs:
- vorticity_new: bfloat16 [32, 2, 136, 768], P('wave', None, 'lev')
- divergence_new: bfloat16 [32, 2, 136, 768], P('wave', None, 'lev')
- temperature_new: bfloat16 [32, 2, 136, 768], P('wave', None, 'lev')
The draws below stay inside these ranges and needn't reach their ends.
All inputs are finite; a program needn't handle non-finite values.
Results may differ from the reference program's by a relative error of at most 0.0075.
Values may be sent and summed in bfloat16 or wider, within the bound.
A program may use at most 64 MiB of HBM per device.

```python
import math
import jax
import jax.numpy as jnp
from jax import lax

DEGREE_LIMIT = 768
STRATA_NUMBER = 136
ORDER_ENTRIES = 32
NQ = 384
N_LEV = 2


def with_ends(drawn, own_key, least, top_value):
    longest = drawn.shape.index(max(drawn.shape))
    spots = []
    for shift in (0, 1):
        where = [jax.random.randint(jax.random.fold_in(own_key, axis), (), 0, length) for axis, length in enumerate(drawn.shape)]
        where[longest] = (where[longest] + shift) % drawn.shape[longest]
        spots.append(tuple(where))
    return drawn.at[spots[0]].set(least).at[spots[1]].set(top_value)


def block_levels(rng, shape, split, low, high):
    loudness, own = 1.0, jax.random.fold_in(rng, 6)
    for position, parts in split:
        steps = jnp.exp(jax.random.uniform(jax.random.fold_in(own, position), (parts,), jnp.float32, low / len(split), high / len(split)))
        loudness = loudness * jnp.repeat(steps, shape[position] // parts).reshape([-1 if axis == position else 1 for axis in range(len(shape))])
    return loudness


def noise(key, extent, scale, most, shards=(), held_as=jnp.bfloat16):
    array = jax.random.normal(key, extent, jnp.float32) * scale
    if len(shards) > 0:
        array = block_levels(key, extent, shards, -0.22, 0.18) * array
    return jnp.clip(array, min=-most, max=most).astype(held_as)


def setup_inputs(seed: int = 0) -> dict:
    key_of = jax.random.split(jax.random.key(seed), 8)
    return {
        "spin_tendency": noise(key_of[0], (ORDER_ENTRIES, 2, STRATA_NUMBER, DEGREE_LIMIT), 1.0, 6.0, ((0, 16), (2, 2))),
        "spreading_source": noise(key_of[1], (ORDER_ENTRIES, 2, STRATA_NUMBER, DEGREE_LIMIT), 1.0, 6.0, ((0, 16), (2, 2))),
        "heat_source": noise(key_of[2], (ORDER_ENTRIES, 2, STRATA_NUMBER, DEGREE_LIMIT), 1.0, 6.0, ((0, 16), (2, 2))),
        "helmholtz_inverses": noise(key_of[3], (N_LEV, NQ, STRATA_NUMBER, STRATA_NUMBER), STRATA_NUMBER ** -0.5, 0.5, ((0, 2), (1, 16))),
        "heat_spreading_coupler": noise(key_of[4], (STRATA_NUMBER, STRATA_NUMBER), STRATA_NUMBER ** -0.5, 0.5),
        "smoothing_strengths": jnp.clip(jnp.exp(jax.random.uniform(key_of[5], (STRATA_NUMBER,), jnp.float32, math.log(0.5), math.log(30.0))), 0.5, 30.0),
        "azimuthal_order_list": with_ends(jax.random.randint(key_of[6], (ORDER_ENTRIES,), 0, DEGREE_LIMIT), jax.random.fold_in(key_of[6], 1), 0, DEGREE_LIMIT - 1).astype(jnp.int32),
    }


def damping_table(smoothing_strengths, wavenumbers):
    scaled = (wavenumbers * (wavenumbers + 1)).astype(jnp.float32) / jnp.float32((DEGREE_LIMIT - 1) * DEGREE_LIMIT)
    return 1.0 / (1.0 + smoothing_strengths.astype(jnp.float32)[:, None] * scaled[None, :] ** 2)


def reference(spin_tendency, spreading_source, heat_source, helmholtz_inverses, heat_spreading_coupler, smoothing_strengths, azimuthal_order_list):
    matrices = helmholtz_inverses.reshape(DEGREE_LIMIT, STRATA_NUMBER, STRATA_NUMBER).astype(jnp.float32)
    blending_matrix = heat_spreading_coupler.astype(jnp.float32)
    wavenumbers = jnp.arange(DEGREE_LIMIT, dtype=jnp.int32)
    damping = damping_table(smoothing_strengths, wavenumbers)

    def lone_order_entry(members):
        rhs_div, rhs_temp, rhs_vort, zonal = members
        answer_fields = jnp.einsum("nkp,cpn->ckn", matrices, rhs_div.astype(jnp.float32)).astype(jnp.bfloat16)
        coupled = jnp.einsum("kp,cpn->ckn", blending_matrix, answer_fields.astype(jnp.float32)).astype(jnp.bfloat16)
        temp_new = (rhs_temp.astype(jnp.float32) - coupled.astype(jnp.float32)).astype(jnp.bfloat16)
        vort_new = (rhs_vort.astype(jnp.float32) * damping[None]).astype(jnp.bfloat16)
        interior_slice = (wavenumbers >= zonal)[None, None, :]
        empty_placeholder = jnp.zeros((), jnp.bfloat16)
        return (jnp.where(interior_slice, vort_new, empty_placeholder), jnp.where(interior_slice, answer_fields, empty_placeholder), jnp.where(interior_slice, temp_new, empty_placeholder))

    spin_updated, spreading_updated, heat_updated = lax.map(lone_order_entry, (spreading_source, heat_source, spin_tendency, azimuthal_order_list))
    return (spin_updated, spreading_updated, heat_updated)
```

```python
import jax
import jax.numpy as jnp
from jax import lax
from jax.sharding import PartitionSpec as P


def damping_table(level_gain, wavenumbers, total_n):
    scaled = (wavenumbers * (wavenumbers + 1)).astype(jnp.float32) / jnp.float32(
        (total_n - 1) * total_n
    )
    return 1.0 / (1.0 + level_gain[:, None] * scaled[None, :] ** 2)


def on_device(
    spin_tendency,
    spreading_source,
    heat_source,
    helmholtz_inverses,
    heat_spreading_coupler,
    smoothing_strengths,
    azimuthal_order_list,
):
    lev_count = lax.axis_size("lev")
    lev_index = lax.axis_index("lev")
    row_count, part_count, lev_local, total_n = spreading_source.shape
    block_n = total_n // lev_count
    layer_count = lev_local * lev_count
    flat_rows = row_count * part_count
    empty_placeholder = jnp.zeros((), jnp.bfloat16)
    wave_count = lax.axis_size("wave")
    local_n = block_n // wave_count
    rhs_div = lax.all_to_all(spreading_source, "lev", split_axis=3, concat_axis=2, tiled=True)
    outgoing = rhs_div.reshape(flat_rows, layer_count, wave_count, local_n).transpose(2, 3, 0, 1)
    outgoing = outgoing.reshape(wave_count, local_n, flat_rows * layer_count)
    columns = lax.all_to_all(outgoing, "wave", split_axis=0, concat_axis=0, tiled=True)
    columns = columns.reshape(wave_count, local_n, flat_rows, layer_count)
    solved_columns = jnp.einsum(
        "jkp,wjcp->wjck", helmholtz_inverses[0], columns, preferred_element_type=jnp.float32
    ).astype(jnp.bfloat16)
    solved_columns = solved_columns.reshape(wave_count, local_n, flat_rows * layer_count)
    returned = lax.all_to_all(solved_columns, "wave", split_axis=0, concat_axis=0, tiled=True)
    answer_fields = returned.reshape(block_n, flat_rows, layer_count).transpose(1, 2, 0)
    coupled = jnp.einsum(
        "om,dms->dos", heat_spreading_coupler, answer_fields, preferred_element_type=jnp.float32
    ).astype(jnp.bfloat16)
    both = jnp.stack([answer_fields, coupled])
    both = lax.all_to_all(both, "lev", split_axis=2, concat_axis=3, tiled=True)
    both = both.reshape(2, row_count, part_count, lev_local, total_n)
    spreading_updated, coupled_out = both[0], both[1]
    heat_updated = (heat_source.astype(jnp.float32) - coupled_out.astype(jnp.float32)).astype(
        jnp.bfloat16
    )
    level_gain = lax.dynamic_slice_in_dim(smoothing_strengths, lev_index * lev_local, lev_local)
    damping = damping_table(level_gain, jnp.arange(total_n, dtype=jnp.int32), total_n)
    spin_updated = (spin_tendency.astype(jnp.float32) * damping[None, None]).astype(jnp.bfloat16)
    interior_slice = (
        jnp.arange(total_n, dtype=jnp.int32)[None, :] >= azimuthal_order_list[:, None]
    )[:, None, None, :]
    return (
        jnp.where(interior_slice, spin_updated, empty_placeholder),
        jnp.where(interior_slice, spreading_updated, empty_placeholder),
        jnp.where(interior_slice, heat_updated, empty_placeholder),
    )


def solution(mesh):
    return jax.shard_map(
        on_device,
        mesh=mesh,
        in_specs=(
            P("wave", None, "lev", None),
            P("wave", None, "lev", None),
            P("wave", None, "lev", None),
            P("lev", "wave", None, None),
            P(),
            P(),
            P("wave"),
        ),
        out_specs=(
            P("wave", None, "lev", None),
            P("wave", None, "lev", None),
            P("wave", None, "lev", None),
        ),
        check_vma=False,
    )
```

```python
import functools
import jax
import jax.numpy as jnp
from jax import lax
from jax.experimental import pallas as pl
from jax.experimental.pallas import tpu as pltpu
from jax.sharding import PartitionSpec as P

LANES = 128
MESH = pl.DeviceIdType.MESH
NT = (((1,), (1,)), ((), ()))
TN = (((0,), (0,)), ((), ()))


def damping_table(level_gain, wavenumbers, total_n):
    scaled = (wavenumbers * (wavenumbers + 1)).astype(jnp.float32) / jnp.float32(
        (total_n - 1) * total_n
    )
    return 1.0 / (1.0 + level_gain[:, None] * scaled[None, :] ** 2)


def exchange_by_collectives(spreading_source, helmholtz_inverses, heat_spreading_coupler):
    lev_count = lax.axis_size("lev")
    row_count, part_count, lev_local, total_n = spreading_source.shape
    block_n = total_n // lev_count
    layer_count = lev_local * lev_count
    flat_rows = row_count * part_count
    wave_count = lax.axis_size("wave")
    local_n = block_n // wave_count
    rhs_div = lax.all_to_all(spreading_source, "lev", split_axis=3, concat_axis=2, tiled=True)
    outgoing = rhs_div.reshape(flat_rows, layer_count, wave_count, local_n).transpose(2, 3, 0, 1)
    outgoing = outgoing.reshape(wave_count, local_n, flat_rows * layer_count)
    columns = lax.all_to_all(outgoing, "wave", split_axis=0, concat_axis=0, tiled=True)
    columns = columns.reshape(wave_count, local_n, flat_rows, layer_count)
    solved_columns = jnp.einsum(
        "jkp,wjcp->wjck", helmholtz_inverses[0], columns, preferred_element_type=jnp.float32
    ).astype(jnp.bfloat16)
    solved_columns = solved_columns.reshape(wave_count, local_n, flat_rows * layer_count)
    returned = lax.all_to_all(solved_columns, "wave", split_axis=0, concat_axis=0, tiled=True)
    answer_fields = returned.reshape(block_n, flat_rows, layer_count).transpose(1, 2, 0)
    coupled = jnp.einsum(
        "om,dms->dos", heat_spreading_coupler, answer_fields, preferred_element_type=jnp.float32
    ).astype(jnp.bfloat16)
    both = jnp.stack([answer_fields, coupled])
    both = lax.all_to_all(both, "lev", split_axis=2, concat_axis=3, tiled=True)
    both = both.reshape(2, row_count, part_count, lev_local, total_n)
    spreading_updated, coupled_out = both[0], both[1]
    return spreading_updated, coupled_out


def f32_dot(left, right, dims):
    return lax.dot_general(left, right, dims, preferred_element_type=jnp.float32)


def exchange_kernel(
    wave_count, lev_count, source, matrices, proj, solved_out, coupled_out,
    halves, outgoing, columns, gathered, strided, returning, returned, results,
    lev_send, lev_recv, wave_send, wave_recv, back_send, back_recv, last_send, last_recv,
):
    wave, lev = lax.axis_index("wave"), lax.axis_index("lev")
    flat_rows, lev_local, total_n = source.shape
    block_n = total_n // lev_count
    local_n = block_n // wave_count
    layer_count = lev_local * lev_count
    extra = layer_count - LANES
    main_lanes = flat_rows * LANES
    wave_peers = [lax.rem(wave + s, wave_count) for s in range(1, wave_count)]
    lev_peers = [lax.rem(lev + s, lev_count) for s in range(1, lev_count)]

    barrier = pltpu.get_barrier_semaphore()
    for peer in wave_peers:
        pl.semaphore_signal(barrier, inc=1, device_id=(peer, lev), device_id_type=MESH)
    for peer in lev_peers:
        pl.semaphore_signal(barrier, inc=1, device_id=(wave, peer), device_id_type=MESH)
    pl.semaphore_wait(barrier, wave_count + lev_count - 2)

    def block_of(index):
        return pl.ds(pl.multiple_of(index * block_n, LANES), block_n)

    lev_copies = []
    for s, peer in enumerate(lev_peers):
        copy = pltpu.make_async_remote_copy(
            src_ref=source.at[:, :, block_of(peer)], dst_ref=halves.at[s],
            send_sem=lev_send.at[s], recv_sem=lev_recv.at[s],
            device_id=(wave, peer), device_id_type=MESH,
        )
        copy.start()
        lev_copies.append(copy)

    def placed(row):
        wide = proj[row]
        first = wide[:, :LANES].astype(jnp.bfloat16)
        rest = wide[:, LANES:]
        out = []
        for r in range(flat_rows):
            rolled = pltpu.roll(rest, r * extra, 1) if r else rest
            out.append(jnp.concatenate([first, rolled.astype(jnp.bfloat16)], axis=1))
        return out

    mine = placed(2 * lev)
    mains = [f32_dot(source[r, :, block_of(lev)], mine[r], TN) for r in range(flat_rows)]
    for s in range(lev_count - 1):
        lev_copies[s].wait()
        theirs = placed(2 * lax.rem(lev + lev_count - 1 - s, lev_count))
        for r in range(flat_rows):
            mains[r] += f32_dot(halves[s, r], theirs[r], TN)
    rests = sum(m[:, LANES:] for m in mains)
    packed = jnp.concatenate([m[:, :LANES] for m in mains] + [rests], axis=1)
    outgoing[...] = packed.reshape(wave_count, local_n, main_lanes + LANES).astype(jnp.bfloat16)

    def exchange(src, dst, send_sems, recv_sems):
        copies = []
        for s, peer in enumerate(wave_peers):
            copy = pltpu.make_async_remote_copy(
                src_ref=src.at[peer], dst_ref=dst.at[wave],
                send_sem=send_sems.at[s], recv_sem=recv_sems.at[s],
                device_id=(peer, lev), device_id_type=MESH,
            )
            copy.start()
            copies.append(copy)
        return copies

    copies = exchange(outgoing, columns, wave_send, wave_recv)
    columns[wave] = outgoing[wave]
    for copy in copies:
        copy.wait()
    for w in range(wave_count):
        for t in range(flat_rows + 1):
            tile = columns[w, :, t * LANES:(t + 1) * LANES]
            gathered[t, pl.ds(w * local_n, local_n), :] = tile.astype(jnp.float32)

    lane = lax.broadcasted_iota(jnp.int32, (wave_count, LANES), 1)

    def solve(j, carry):
        rows = pl.ds(j, wave_count, stride=local_n)
        rest = gathered[flat_rows, rows, :]
        parts = []
        for r in range(flat_rows):
            rolled = pltpu.roll(rest, LANES - r * extra, 1) if r else rest
            main = gathered[r, rows, :]
            parts.append(jnp.concatenate([main, rolled], axis=1)[:, :layer_count])
        stacked = jnp.concatenate(parts, axis=0).astype(jnp.bfloat16)
        main = f32_dot(stacked, matrices[j, :LANES, :], NT)
        last = f32_dot(stacked, matrices[j, layer_count - LANES:, :], NT)
        rest = jnp.zeros((wave_count, LANES), jnp.float32)
        for r in range(flat_rows):
            strided[r, rows, :] = main[r * wave_count:(r + 1) * wave_count]
            rolled = pltpu.roll(last[r * wave_count:(r + 1) * wave_count], (r + 1) * extra, 1)
            keep = (lane >= r * extra) & (lane < (r + 1) * extra)
            rest = jnp.where(keep, rolled, rest)
        strided[flat_rows, rows, :] = rest
        return carry

    lax.fori_loop(0, local_n, solve, 0, unroll=4)
    for w in range(wave_count):
        for t in range(flat_rows + 1):
            tile = strided[t, pl.ds(w * local_n, local_n), :]
            returning[w, :, t * LANES:(t + 1) * LANES] = tile.astype(jnp.bfloat16)

    copies = exchange(returning, returned, back_send, back_recv)
    returned[wave] = returning[wave]
    for copy in copies:
        copy.wait()
    back = returned[...].astype(jnp.float32).reshape(block_n, main_lanes + LANES)
    back = back.astype(jnp.bfloat16)

    def finish(row):
        out = []
        for r, weights in enumerate(placed(row)):
            pair = jnp.concatenate(
                [back[:, r * LANES:(r + 1) * LANES], back[:, main_lanes:]], axis=1
            )
            out.append(f32_dot(weights, pair, NT).astype(jnp.bfloat16))
        return out

    copies = []
    for s, peer in enumerate(lev_peers):
        for field, target in enumerate((solved_out, coupled_out)):
            for r, value in enumerate(finish(2 * peer + field)):
                results[s, field, r] = value
            copy = pltpu.make_async_remote_copy(
                src_ref=results.at[s, field], dst_ref=target.at[:, :, block_of(lev)],
                send_sem=last_send.at[s, field], recv_sem=last_recv.at[s, field],
                device_id=(wave, peer), device_id_type=MESH,
            )
            copy.start()
            copies.append(copy)
    for field, target in enumerate((solved_out, coupled_out)):
        for r, value in enumerate(finish(2 * lev + field)):
            target[r, :, block_of(lev)] = value
    for copy in copies:
        copy.wait()


def exchange_by_kernel(spreading_source, helmholtz_inverses, heat_spreading_coupler):
    lev_count, wave_count = lax.axis_size("lev"), lax.axis_size("wave")
    row_count, part_count, lev_local, total_n = spreading_source.shape
    block_n = total_n // lev_count
    local_n = block_n // wave_count
    layer_count = lev_local * lev_count
    flat_rows = row_count * part_count
    width = (flat_rows + 1) * LANES
    proj = jnp.stack([jnp.eye(layer_count, dtype=jnp.float32), heat_spreading_coupler.astype(jnp.float32)])
    proj = jnp.pad(proj, ((0, 0), (0, 0), (0, 2 * LANES - layer_count)))
    proj = proj.reshape(2, lev_count, lev_local, 2 * LANES).transpose(1, 0, 2, 3)
    proj = proj.reshape(2 * lev_count, lev_local, 2 * LANES)
    vmem = pl.BlockSpec(memory_space=pltpu.VMEM)
    field = jax.ShapeDtypeStruct((flat_rows, lev_local, total_n), jnp.bfloat16)
    wire = pltpu.VMEM((wave_count, local_n, width), jnp.bfloat16)
    wide = pltpu.VMEM((flat_rows + 1, block_n, LANES), jnp.float32)
    dma = pltpu.SemaphoreType.DMA
    solved, coupled = pl.pallas_call(
        functools.partial(exchange_kernel, wave_count, lev_count),
        out_shape=(field, field),
        in_specs=[vmem] * 3,
        out_specs=(vmem, vmem),
        scratch_shapes=[
            pltpu.VMEM((lev_count - 1, flat_rows, lev_local, block_n), jnp.bfloat16),
            wire, wire, wide, wide, wire, wire,
            pltpu.VMEM((lev_count - 1, 2, flat_rows, lev_local, block_n), jnp.bfloat16),
            dma((lev_count - 1,)), dma((lev_count - 1,)),
            dma((wave_count - 1,)), dma((wave_count - 1,)),
            dma((wave_count - 1,)), dma((wave_count - 1,)),
            dma((lev_count - 1, 2)), dma((lev_count - 1, 2)),
        ],
        compiler_params=pltpu.CompilerParams(
            collective_id=0, has_side_effects=True, vmem_limit_bytes=48 * 2**20
        ),
    )(spreading_source.reshape(field.shape), helmholtz_inverses[0], proj)
    shape = spreading_source.shape
    return solved.reshape(shape), coupled.reshape(shape)


def kernel_fits(source_shape, lev_count, wave_count):
    row_count, part_count, lev_local, total_n = source_shape
    block_n = total_n // lev_count
    extra = lev_local * lev_count - LANES
    return (
        lev_count > 1
        and wave_count > 1
        and wave_count % 8 == 0
        and block_n % LANES == 0
        and block_n % (8 * wave_count) == 0
        and extra > 0
        and extra * row_count * part_count <= LANES
    )


def on_device(
    spin_tendency,
    spreading_source,
    heat_source,
    helmholtz_inverses,
    heat_spreading_coupler,
    smoothing_strengths,
    azimuthal_order_list,
):
    lev_count, wave_count = lax.axis_size("lev"), lax.axis_size("wave")
    lev_index = lax.axis_index("lev")
    lev_local, total_n = spreading_source.shape[2:]
    empty_placeholder = jnp.zeros((), jnp.bfloat16)
    fits = kernel_fits(spreading_source.shape, lev_count, wave_count)
    exchange = exchange_by_kernel if fits else exchange_by_collectives
    spreading_updated, coupled_out = exchange(
        spreading_source, helmholtz_inverses, heat_spreading_coupler
    )
    heat_updated = (heat_source.astype(jnp.float32) - coupled_out.astype(jnp.float32)).astype(
        jnp.bfloat16
    )
    level_gain = lax.dynamic_slice_in_dim(smoothing_strengths, lev_index * lev_local, lev_local)
    damping = damping_table(level_gain, jnp.arange(total_n, dtype=jnp.int32), total_n)
    spin_updated = (spin_tendency.astype(jnp.float32) * damping[None, None]).astype(jnp.bfloat16)
    interior_slice = (
        jnp.arange(total_n, dtype=jnp.int32)[None, :] >= azimuthal_order_list[:, None]
    )[:, None, None, :]
    return (
        jnp.where(interior_slice, spin_updated, empty_placeholder),
        jnp.where(interior_slice, spreading_updated, empty_placeholder),
        jnp.where(interior_slice, heat_updated, empty_placeholder),
    )


def solution(mesh):
    return jax.shard_map(
        on_device,
        mesh=mesh,
        in_specs=(
            P("wave", None, "lev", None),
            P("wave", None, "lev", None),
            P("wave", None, "lev", None),
            P("lev", "wave", None, None),
            P(),
            P(),
            P("wave"),
        ),
        out_specs=(
            P("wave", None, "lev", None),
            P("wave", None, "lev", None),
            P("wave", None, "lev", None),
        ),
        check_vma=False,
    )
```

```python
import functools
import jax
import jax.numpy as jnp
from jax import lax
from jax.experimental import pallas as pl
from jax.experimental.pallas import tpu as pltpu
from jax.sharding import PartitionSpec as P

LANES = 128
MESH = pl.DeviceIdType.MESH
NT = (((1,), (1,)), ((), ()))
TN = (((0,), (0,)), ((), ()))


def damping_table(level_gain, wavenumbers, total_n):
    scaled = (wavenumbers * (wavenumbers + 1)).astype(jnp.float32) / jnp.float32(
        (total_n - 1) * total_n
    )
    return 1.0 / (1.0 + level_gain[:, None] * scaled[None, :] ** 2)


def exchange_by_collectives(spreading_source, helmholtz_inverses, heat_spreading_coupler):
    lev_count = lax.axis_size("lev")
    row_count, part_count, lev_local, total_n = spreading_source.shape
    block_n = total_n // lev_count
    layer_count = lev_local * lev_count
    flat_rows = row_count * part_count
    wave_count = lax.axis_size("wave")
    local_n = block_n // wave_count
    rhs_div = lax.all_to_all(spreading_source, "lev", split_axis=3, concat_axis=2, tiled=True)
    outgoing = rhs_div.reshape(flat_rows, layer_count, wave_count, local_n).transpose(2, 3, 0, 1)
    outgoing = outgoing.reshape(wave_count, local_n, flat_rows * layer_count)
    columns = lax.all_to_all(outgoing, "wave", split_axis=0, concat_axis=0, tiled=True)
    columns = columns.reshape(wave_count, local_n, flat_rows, layer_count)
    solved_columns = jnp.einsum(
        "jkp,wjcp->wjck", helmholtz_inverses[0], columns, preferred_element_type=jnp.float32
    ).astype(jnp.bfloat16)
    solved_columns = solved_columns.reshape(wave_count, local_n, flat_rows * layer_count)
    returned = lax.all_to_all(solved_columns, "wave", split_axis=0, concat_axis=0, tiled=True)
    answer_fields = returned.reshape(block_n, flat_rows, layer_count).transpose(1, 2, 0)
    coupled = jnp.einsum(
        "om,dms->dos", heat_spreading_coupler, answer_fields, preferred_element_type=jnp.float32
    ).astype(jnp.bfloat16)
    both = jnp.stack([answer_fields, coupled])
    both = lax.all_to_all(both, "lev", split_axis=2, concat_axis=3, tiled=True)
    both = both.reshape(2, row_count, part_count, lev_local, total_n)
    spreading_updated, coupled_out = both[0], both[1]
    return spreading_updated, coupled_out


def f32_dot(left, right, dims):
    return lax.dot_general(left, right, dims, preferred_element_type=jnp.float32)


def chunk_rows(flat_rows):
    size = max(1, flat_rows // 2)
    return [range(r, min(r + size, flat_rows)) for r in range(0, flat_rows, size)]


def exchange_kernel(wave_count, lev_count, chunks, source, matrices, proj, solved_out, coupled_out, *scratch):
    count = len(chunks)
    halves, gathered, strided, results = scratch[:4]
    outgoing, columns, returning, returned = (
        scratch[4 + k * count:4 + (k + 1) * count] for k in range(4)
    )
    (lev_send, lev_recv, wave_send, wave_recv, back_send, back_recv, last_send, last_recv) = scratch[
        4 + 4 * count:
    ]
    wave, lev = lax.axis_index("wave"), lax.axis_index("lev")
    flat_rows, lev_local, total_n = source.shape
    block_n = total_n // lev_count
    local_n = block_n // wave_count
    groups = local_n // 8
    layer_count = lev_local * lev_count
    extra = layer_count - LANES
    wave_peers = [lax.rem(wave + s, wave_count) for s in range(1, wave_count)]
    lev_peers = [lax.rem(lev + s, lev_count) for s in range(1, lev_count)]

    barrier = pltpu.get_barrier_semaphore()
    for peer in wave_peers:
        pl.semaphore_signal(barrier, inc=1, device_id=(peer, lev), device_id_type=MESH)
    for peer in lev_peers:
        pl.semaphore_signal(barrier, inc=1, device_id=(wave, peer), device_id_type=MESH)
    pl.semaphore_wait(barrier, wave_count + lev_count - 2)

    def block_of(index):
        return pl.ds(pl.multiple_of(index * block_n, LANES), block_n)

    def rows_of(c):
        return pl.ds(chunks[c][0], len(chunks[c]))

    lev_copies = []
    for c in range(count):
        for s, peer in enumerate(lev_peers):
            copy = pltpu.make_async_remote_copy(
                src_ref=source.at[rows_of(c), :, block_of(peer)], dst_ref=halves.at[s, rows_of(c)],
                send_sem=lev_send.at[s, c], recv_sem=lev_recv.at[s, c],
                device_id=(wave, peer), device_id_type=MESH,
            )
            copy.start()
            lev_copies.append(copy)

    def shifted(tile, amount):
        amount = amount % LANES
        return pltpu.roll(tile, amount, 1) if amount else tile

    def placed(row, size):
        wide = proj[row]
        first = wide[:, :LANES].astype(jnp.bfloat16)
        rest = wide[:, LANES:]
        return [
            jnp.concatenate([first, shifted(rest, i * extra).astype(jnp.bfloat16)], axis=1)
            for i in range(size)
        ]

    def pack(mains, rest, step):
        rest = rest.reshape(wave_count, groups, 8, LANES)
        folded = rest[:, 0].reshape(wave_count * 8, LANES)
        for g in range(1, groups):
            folded += shifted(rest[:, g].reshape(wave_count * 8, LANES), g * step)
        pieces = [m.reshape(wave_count, local_n, LANES) for m in mains]
        pieces.append(folded.reshape(wave_count, 8, LANES))
        return jnp.concatenate(pieces, axis=1).astype(jnp.bfloat16)

    def unpack(wire, size):
        step = size * extra
        value = wire[...].astype(jnp.float32)
        mains = [
            value[:, i * local_n:(i + 1) * local_n].reshape(block_n, LANES) for i in range(size)
        ]
        folded = value[:, size * local_n:].reshape(wave_count * 8, LANES)
        rest = [
            shifted(folded, -g * step).reshape(wave_count, 1, 8, LANES) for g in range(groups)
        ]
        return mains, jnp.concatenate(rest, axis=1).reshape(block_n, LANES)

    def exchange(src, dst, send_sems, recv_sems, c):
        copies = []
        for s, peer in enumerate(wave_peers):
            copy = pltpu.make_async_remote_copy(
                src_ref=src[c].at[peer], dst_ref=dst[c].at[wave],
                send_sem=send_sems.at[s, c], recv_sem=recv_sems.at[s, c],
                device_id=(peer, lev), device_id_type=MESH,
            )
            copy.start()
            copies.append(copy)
        dst[c][wave] = src[c][wave]
        return copies

    lane = lax.broadcasted_iota(jnp.int32, (wave_count, LANES), 1)
    out_copies, back_copies, last_copies = [], [], []
    for c, chunk in enumerate(chunks):
        size = len(chunk)
        mine = placed(2 * lev, size)
        sums = [f32_dot(source[r, :, block_of(lev)], mine[i], TN) for i, r in enumerate(chunk)]
        for s in range(lev_count - 1):
            lev_copies[c * (lev_count - 1) + s].wait()
            theirs = placed(2 * lax.rem(lev + lev_count - 1 - s, lev_count), size)
            for i, r in enumerate(chunk):
                sums[i] += f32_dot(halves[s, r], theirs[i], TN)
        rest = sum(m[:, LANES:] for m in sums)
        outgoing[c][...] = pack([m[:, :LANES] for m in sums], rest, size * extra)
        out_copies.append(exchange(outgoing, columns, wave_send, wave_recv, c))

    for c, chunk in enumerate(chunks):
        size = len(chunk)
        for copy in out_copies[c]:
            copy.wait()
        mains, rest = unpack(columns[c], size)
        for i, main in enumerate(mains):
            gathered[i] = main
        gathered[size] = rest

        def solve(j, carry):
            rows = pl.ds(j, wave_count, stride=local_n)
            rest = gathered[size, rows, :]
            parts = []
            for i in range(size):
                both = [gathered[i, rows, :], shifted(rest, -i * extra)]
                parts.append(jnp.concatenate(both, axis=1)[:, :layer_count])
            stacked = jnp.concatenate(parts, axis=0).astype(jnp.bfloat16)
            main = f32_dot(stacked, matrices[j, :LANES, :], NT)
            last = f32_dot(stacked, matrices[j, layer_count - LANES:, :], NT)
            rest = jnp.zeros((wave_count, LANES), jnp.float32)
            for i in range(size):
                part = slice(i * wave_count, (i + 1) * wave_count)
                strided[i, rows, :] = main[part]
                keep = (lane >= i * extra) & (lane < (i + 1) * extra)
                rest = jnp.where(keep, shifted(last[part], (i + 1) * extra), rest)
            strided[size, rows, :] = rest
            return carry

        lax.fori_loop(0, local_n, solve, 0, unroll=4)
        returning[c][...] = pack([strided[i] for i in range(size)], strided[size], size * extra)
        back_copies.append(exchange(returning, returned, back_send, back_recv, c))

    for c, chunk in enumerate(chunks):
        size = len(chunk)
        for copy in back_copies[c]:
            copy.wait()
        mains, rest = unpack(returned[c], size)
        pairs = [jnp.concatenate([main, rest], axis=1).astype(jnp.bfloat16) for main in mains]

        def finish(row):
            return [
                f32_dot(weights, pair, NT).astype(jnp.bfloat16)
                for weights, pair in zip(placed(row, size), pairs)
            ]

        for s, peer in enumerate(lev_peers):
            for field, target in enumerate((solved_out, coupled_out)):
                for r, value in zip(chunk, finish(2 * peer + field)):
                    results[s, field, r] = value
                copy = pltpu.make_async_remote_copy(
                    src_ref=results.at[s, field, rows_of(c)],
                    dst_ref=target.at[rows_of(c), :, block_of(lev)],
                    send_sem=last_send.at[s, field, c], recv_sem=last_recv.at[s, field, c],
                    device_id=(wave, peer), device_id_type=MESH,
                )
                copy.start()
                last_copies.append(copy)
        for field, target in enumerate((solved_out, coupled_out)):
            for r, value in zip(chunk, finish(2 * lev + field)):
                target[r, :, block_of(lev)] = value
    for copy in last_copies:
        copy.wait()


def exchange_by_kernel(spreading_source, helmholtz_inverses, heat_spreading_coupler):
    lev_count, wave_count = lax.axis_size("lev"), lax.axis_size("wave")
    row_count, part_count, lev_local, total_n = spreading_source.shape
    block_n = total_n // lev_count
    local_n = block_n // wave_count
    layer_count = lev_local * lev_count
    flat_rows = row_count * part_count
    chunks = chunk_rows(flat_rows)
    longest = max(len(chunk) for chunk in chunks)
    proj = jnp.stack([jnp.eye(layer_count, dtype=jnp.float32), heat_spreading_coupler.astype(jnp.float32)])
    proj = jnp.pad(proj, ((0, 0), (0, 0), (0, 2 * LANES - layer_count)))
    proj = proj.reshape(2, lev_count, lev_local, 2 * LANES).transpose(1, 0, 2, 3)
    proj = proj.reshape(2 * lev_count, lev_local, 2 * LANES)
    vmem = pl.BlockSpec(memory_space=pltpu.VMEM)
    field = jax.ShapeDtypeStruct((flat_rows, lev_local, total_n), jnp.bfloat16)
    wires = [pltpu.VMEM((wave_count, len(c) * local_n + 8, LANES), jnp.bfloat16) for c in chunks]
    wide = pltpu.VMEM((longest + 1, block_n, LANES), jnp.float32)
    dma = pltpu.SemaphoreType.DMA
    lev_sems, wave_sems = dma((lev_count - 1, len(chunks))), dma((wave_count - 1, len(chunks)))
    last_sems = dma((lev_count - 1, 2, len(chunks)))
    solved, coupled = pl.pallas_call(
        functools.partial(exchange_kernel, wave_count, lev_count, chunks),
        out_shape=(field, field),
        in_specs=[vmem] * 3,
        out_specs=(vmem, vmem),
        scratch_shapes=[
            pltpu.VMEM((lev_count - 1, flat_rows, lev_local, block_n), jnp.bfloat16),
            wide, wide,
            pltpu.VMEM((lev_count - 1, 2, flat_rows, lev_local, block_n), jnp.bfloat16),
            *wires, *wires, *wires, *wires,
            lev_sems, lev_sems, wave_sems, wave_sems, wave_sems, wave_sems, last_sems, last_sems,
        ],
        compiler_params=pltpu.CompilerParams(
            collective_id=0, has_side_effects=True, vmem_limit_bytes=48 * 2**20
        ),
    )(spreading_source.reshape(field.shape), helmholtz_inverses[0], proj)
    shape = spreading_source.shape
    return solved.reshape(shape), coupled.reshape(shape)


def kernel_fits(source_shape, lev_count, wave_count):
    row_count, part_count, lev_local, total_n = source_shape
    block_n = total_n // lev_count
    extra = lev_local * lev_count - LANES
    return (
        lev_count > 1
        and wave_count > 1
        and wave_count % 8 == 0
        and block_n % LANES == 0
        and block_n % (8 * wave_count) == 0
        and extra > 0
        and extra * row_count * part_count * (block_n // (8 * wave_count)) <= LANES
    )


def on_device(
    spin_tendency,
    spreading_source,
    heat_source,
    helmholtz_inverses,
    heat_spreading_coupler,
    smoothing_strengths,
    azimuthal_order_list,
):
    lev_count, wave_count = lax.axis_size("lev"), lax.axis_size("wave")
    lev_index = lax.axis_index("lev")
    lev_local, total_n = spreading_source.shape[2:]
    empty_placeholder = jnp.zeros((), jnp.bfloat16)
    fits = kernel_fits(spreading_source.shape, lev_count, wave_count)
    exchange = exchange_by_kernel if fits else exchange_by_collectives
    spreading_updated, coupled_out = exchange(
        spreading_source, helmholtz_inverses, heat_spreading_coupler
    )
    heat_updated = (heat_source.astype(jnp.float32) - coupled_out.astype(jnp.float32)).astype(
        jnp.bfloat16
    )
    level_gain = lax.dynamic_slice_in_dim(smoothing_strengths, lev_index * lev_local, lev_local)
    damping = damping_table(level_gain, jnp.arange(total_n, dtype=jnp.int32), total_n)
    spin_updated = (spin_tendency.astype(jnp.float32) * damping[None, None]).astype(jnp.bfloat16)
    interior_slice = (
        jnp.arange(total_n, dtype=jnp.int32)[None, :] >= azimuthal_order_list[:, None]
    )[:, None, None, :]
    return (
        jnp.where(interior_slice, spin_updated, empty_placeholder),
        jnp.where(interior_slice, spreading_updated, empty_placeholder),
        jnp.where(interior_slice, heat_updated, empty_placeholder),
    )


def solution(mesh):
    return jax.shard_map(
        on_device,
        mesh=mesh,
        in_specs=(
            P("wave", None, "lev", None),
            P("wave", None, "lev", None),
            P("wave", None, "lev", None),
            P("lev", "wave", None, None),
            P(),
            P(),
            P("wave"),
        ),
        out_specs=(
            P("wave", None, "lev", None),
            P("wave", None, "lev", None),
            P("wave", None, "lev", None),
        ),
        check_vma=False,
    )
```

```python
import functools
import jax
import jax.numpy as jnp
from jax import lax
from jax.experimental import pallas as pl
from jax.experimental.pallas import tpu as pltpu
from jax.sharding import PartitionSpec as P

LANES = 128
MESH = pl.DeviceIdType.MESH
NT = (((1,), (1,)), ((), ()))
TN = (((0,), (0,)), ((), ()))


def damping_table(level_gain, wavenumbers, total_n):
    scaled = (wavenumbers * (wavenumbers + 1)).astype(jnp.float32) / jnp.float32(
        (total_n - 1) * total_n
    )
    return 1.0 / (1.0 + level_gain[:, None] * scaled[None, :] ** 2)


def exchange_by_collectives(spreading_source, helmholtz_inverses, heat_spreading_coupler):
    lev_count = lax.axis_size("lev")
    row_count, part_count, lev_local, total_n = spreading_source.shape
    block_n = total_n // lev_count
    layer_count = lev_local * lev_count
    flat_rows = row_count * part_count
    wave_count = lax.axis_size("wave")
    local_n = block_n // wave_count
    rhs_div = lax.all_to_all(spreading_source, "lev", split_axis=3, concat_axis=2, tiled=True)
    outgoing = rhs_div.reshape(flat_rows, layer_count, wave_count, local_n).transpose(2, 3, 0, 1)
    outgoing = outgoing.reshape(wave_count, local_n, flat_rows * layer_count)
    columns = lax.all_to_all(outgoing, "wave", split_axis=0, concat_axis=0, tiled=True)
    columns = columns.reshape(wave_count, local_n, flat_rows, layer_count)
    solved_columns = jnp.einsum(
        "jkp,wjcp->wjck", helmholtz_inverses[0], columns, preferred_element_type=jnp.float32
    ).astype(jnp.bfloat16)
    solved_columns = solved_columns.reshape(wave_count, local_n, flat_rows * layer_count)
    returned = lax.all_to_all(solved_columns, "wave", split_axis=0, concat_axis=0, tiled=True)
    answer_fields = returned.reshape(block_n, flat_rows, layer_count).transpose(1, 2, 0)
    coupled = jnp.einsum(
        "om,dms->dos", heat_spreading_coupler, answer_fields, preferred_element_type=jnp.float32
    ).astype(jnp.bfloat16)
    both = jnp.stack([answer_fields, coupled])
    both = lax.all_to_all(both, "lev", split_axis=2, concat_axis=3, tiled=True)
    both = both.reshape(2, row_count, part_count, lev_local, total_n)
    spreading_updated, coupled_out = both[0], both[1]
    return spreading_updated, coupled_out


def f32_dot(left, right, dims):
    return lax.dot_general(left, right, dims, preferred_element_type=jnp.float32)


def chunk_rows(flat_rows):
    size = max(1, flat_rows // 4)
    cuts = [0, size, flat_rows - size, flat_rows]
    return [range(lo, hi) for lo, hi in zip(cuts, cuts[1:]) if hi > lo]


def exchange_kernel(wave_count, lev_count, chunks, source, matrices, proj, solved_out, coupled_out, *scratch):
    count = len(chunks)
    halves, gathered, strided, results = scratch[:4]
    outgoing, columns, returning, returned = (
        scratch[4 + k * count:4 + (k + 1) * count] for k in range(4)
    )
    (lev_send, lev_recv, wave_send, wave_recv, back_send, back_recv, last_send, last_recv) = scratch[
        4 + 4 * count:
    ]
    wave, lev = lax.axis_index("wave"), lax.axis_index("lev")
    flat_rows, lev_local, total_n = source.shape
    block_n = total_n // lev_count
    local_n = block_n // wave_count
    groups = local_n // 8
    layer_count = lev_local * lev_count
    extra = layer_count - LANES
    wave_peers = [lax.rem(wave + s, wave_count) for s in sorted(range(1, wave_count), key=lambda s: abs(2 * s - wave_count))]
    lev_peers = [lax.rem(lev + s, lev_count) for s in range(1, lev_count)]

    barrier = pltpu.get_barrier_semaphore()
    for peer in wave_peers:
        pl.semaphore_signal(barrier, inc=1, device_id=(peer, lev), device_id_type=MESH)
    for peer in lev_peers:
        pl.semaphore_signal(barrier, inc=1, device_id=(wave, peer), device_id_type=MESH)
    pl.semaphore_wait(barrier, wave_count + lev_count - 2)

    def block_of(index):
        return pl.ds(pl.multiple_of(index * block_n, LANES), block_n)

    def rows_of(c):
        return pl.ds(chunks[c][0], len(chunks[c]))

    lev_copies = []
    for c in range(count):
        for s, peer in enumerate(lev_peers):
            copy = pltpu.make_async_remote_copy(
                src_ref=source.at[rows_of(c), :, block_of(peer)], dst_ref=halves.at[s, rows_of(c)],
                send_sem=lev_send.at[s, c], recv_sem=lev_recv.at[s, c],
                device_id=(wave, peer), device_id_type=MESH,
            )
            copy.start()
            lev_copies.append(copy)

    def shifted(tile, amount):
        amount = amount % LANES
        return pltpu.roll(tile, amount, 1) if amount else tile

    def placed(row, size):
        wide = proj[row]
        first = wide[:, :LANES].astype(jnp.bfloat16)
        rest = wide[:, LANES:]
        return [
            jnp.concatenate([first, shifted(rest, i * extra).astype(jnp.bfloat16)], axis=1)
            for i in range(size)
        ]

    def pack(mains, rest, step):
        rest = rest.reshape(wave_count, groups, 8, LANES)
        folded = rest[:, 0].reshape(wave_count * 8, LANES)
        for g in range(1, groups):
            folded += shifted(rest[:, g].reshape(wave_count * 8, LANES), g * step)
        pieces = [m.reshape(wave_count, local_n, LANES) for m in mains]
        pieces.append(folded.reshape(wave_count, 8, LANES))
        return jnp.concatenate(pieces, axis=1).astype(jnp.bfloat16)

    def unpack(wire, size):
        step = size * extra
        value = wire[...].astype(jnp.float32)
        mains = [
            value[:, i * local_n:(i + 1) * local_n].reshape(block_n, LANES) for i in range(size)
        ]
        folded = value[:, size * local_n:].reshape(wave_count * 8, LANES)
        rest = [
            shifted(folded, -g * step).reshape(wave_count, 1, 8, LANES) for g in range(groups)
        ]
        return mains, jnp.concatenate(rest, axis=1).reshape(block_n, LANES)

    def exchange(src, dst, send_sems, recv_sems, c):
        copies = []
        for s, peer in enumerate(wave_peers):
            copy = pltpu.make_async_remote_copy(
                src_ref=src[c].at[peer], dst_ref=dst[c].at[wave],
                send_sem=send_sems.at[s, c], recv_sem=recv_sems.at[s, c],
                device_id=(peer, lev), device_id_type=MESH,
            )
            copy.start()
            copies.append(copy)
        dst[c][wave] = src[c][wave]
        return copies

    lane = lax.broadcasted_iota(jnp.int32, (wave_count, LANES), 1)
    out_copies, back_copies, last_copies = [], [], []
    for c, chunk in enumerate(chunks):
        size = len(chunk)
        mine = placed(2 * lev, size)
        sums = [f32_dot(source[r, :, block_of(lev)], mine[i], TN) for i, r in enumerate(chunk)]
        for s in range(lev_count - 1):
            lev_copies[c * (lev_count - 1) + s].wait()
            theirs = placed(2 * lax.rem(lev + lev_count - 1 - s, lev_count), size)
            for i, r in enumerate(chunk):
                sums[i] += f32_dot(halves[s, r], theirs[i], TN)
        rest = sum(m[:, LANES:] for m in sums)
        outgoing[c][...] = pack([m[:, :LANES] for m in sums], rest, size * extra)
        out_copies.append(exchange(outgoing, columns, wave_send, wave_recv, c))

    for c, chunk in enumerate(chunks):
        size = len(chunk)
        for copy in out_copies[c]:
            copy.wait()
        mains, rest = unpack(columns[c], size)
        for i, main in enumerate(mains):
            gathered[i] = main
        gathered[size] = rest

        def solve(j, carry):
            rows = pl.ds(j, wave_count, stride=local_n)
            rest = gathered[size, rows, :]
            parts = []
            for i in range(size):
                both = [gathered[i, rows, :], shifted(rest, -i * extra)]
                parts.append(jnp.concatenate(both, axis=1)[:, :layer_count])
            stacked = jnp.concatenate(parts, axis=0).astype(jnp.bfloat16)
            main = f32_dot(stacked, matrices[j, :LANES, :], NT)
            last = f32_dot(stacked, matrices[j, layer_count - LANES:, :], NT)
            rest = jnp.zeros((wave_count, LANES), jnp.float32)
            for i in range(size):
                part = slice(i * wave_count, (i + 1) * wave_count)
                strided[i, rows, :] = main[part]
                keep = (lane >= i * extra) & (lane < (i + 1) * extra)
                rest = jnp.where(keep, shifted(last[part], (i + 1) * extra), rest)
            strided[size, rows, :] = rest
            return carry

        lax.fori_loop(0, local_n, solve, 0, unroll=8)
        returning[c][...] = pack([strided[i] for i in range(size)], strided[size], size * extra)
        back_copies.append(exchange(returning, returned, back_send, back_recv, c))

    for c, chunk in enumerate(chunks):
        size = len(chunk)
        for copy in back_copies[c]:
            copy.wait()
        mains, rest = unpack(returned[c], size)
        pairs = [jnp.concatenate([main, rest], axis=1).astype(jnp.bfloat16) for main in mains]

        def finish(row):
            return [
                f32_dot(weights, pair, NT).astype(jnp.bfloat16)
                for weights, pair in zip(placed(row, size), pairs)
            ]

        for s, peer in enumerate(lev_peers):
            for field, target in enumerate((solved_out, coupled_out)):
                for r, value in zip(chunk, finish(2 * peer + field)):
                    results[s, field, r] = value
                copy = pltpu.make_async_remote_copy(
                    src_ref=results.at[s, field, rows_of(c)],
                    dst_ref=target.at[rows_of(c), :, block_of(lev)],
                    send_sem=last_send.at[s, field, c], recv_sem=last_recv.at[s, field, c],
                    device_id=(wave, peer), device_id_type=MESH,
                )
                copy.start()
                last_copies.append(copy)
        for field, target in enumerate((solved_out, coupled_out)):
            for r, value in zip(chunk, finish(2 * lev + field)):
                target[r, :, block_of(lev)] = value
    for copy in last_copies:
        copy.wait()


def exchange_by_kernel(spreading_source, helmholtz_inverses, heat_spreading_coupler):
    lev_count, wave_count = lax.axis_size("lev"), lax.axis_size("wave")
    row_count, part_count, lev_local, total_n = spreading_source.shape
    block_n = total_n // lev_count
    local_n = block_n // wave_count
    layer_count = lev_local * lev_count
    flat_rows = row_count * part_count
    chunks = chunk_rows(flat_rows)
    longest = max(len(chunk) for chunk in chunks)
    proj = jnp.stack([jnp.eye(layer_count, dtype=jnp.float32), heat_spreading_coupler.astype(jnp.float32)])
    proj = jnp.pad(proj, ((0, 0), (0, 0), (0, 2 * LANES - layer_count)))
    proj = proj.reshape(2, lev_count, lev_local, 2 * LANES).transpose(1, 0, 2, 3)
    proj = proj.reshape(2 * lev_count, lev_local, 2 * LANES)
    vmem = pl.BlockSpec(memory_space=pltpu.VMEM)
    field = jax.ShapeDtypeStruct((flat_rows, lev_local, total_n), jnp.bfloat16)
    wires = [pltpu.VMEM((wave_count, len(c) * local_n + 8, LANES), jnp.bfloat16) for c in chunks]
    wide = pltpu.VMEM((longest + 1, block_n, LANES), jnp.float32)
    dma = pltpu.SemaphoreType.DMA
    lev_sems, wave_sems = dma((lev_count - 1, len(chunks))), dma((wave_count - 1, len(chunks)))
    last_sems = dma((lev_count - 1, 2, len(chunks)))
    solved, coupled = pl.pallas_call(
        functools.partial(exchange_kernel, wave_count, lev_count, chunks),
        out_shape=(field, field),
        in_specs=[vmem] * 3,
        out_specs=(vmem, vmem),
        scratch_shapes=[
            pltpu.VMEM((lev_count - 1, flat_rows, lev_local, block_n), jnp.bfloat16),
            wide, wide,
            pltpu.VMEM((lev_count - 1, 2, flat_rows, lev_local, block_n), jnp.bfloat16),
            *wires, *wires, *wires, *wires,
            lev_sems, lev_sems, wave_sems, wave_sems, wave_sems, wave_sems, last_sems, last_sems,
        ],
        compiler_params=pltpu.CompilerParams(
            collective_id=0, has_side_effects=True, vmem_limit_bytes=48 * 2**20
        ),
    )(spreading_source.reshape(field.shape), helmholtz_inverses[0], proj)
    shape = spreading_source.shape
    return solved.reshape(shape), coupled.reshape(shape)


def kernel_fits(source_shape, lev_count, wave_count):
    row_count, part_count, lev_local, total_n = source_shape
    block_n = total_n // lev_count
    extra = lev_local * lev_count - LANES
    return (
        lev_count > 1
        and wave_count > 1
        and wave_count % 8 == 0
        and block_n % LANES == 0
        and block_n % (8 * wave_count) == 0
        and extra > 0
        and extra * row_count * part_count * (block_n // (8 * wave_count)) <= LANES
    )


def on_device(
    spin_tendency,
    spreading_source,
    heat_source,
    helmholtz_inverses,
    heat_spreading_coupler,
    smoothing_strengths,
    azimuthal_order_list,
):
    lev_count, wave_count = lax.axis_size("lev"), lax.axis_size("wave")
    lev_index = lax.axis_index("lev")
    lev_local, total_n = spreading_source.shape[2:]
    empty_placeholder = jnp.zeros((), jnp.bfloat16)
    fits = kernel_fits(spreading_source.shape, lev_count, wave_count)
    exchange = exchange_by_kernel if fits else exchange_by_collectives
    spreading_updated, coupled_out = exchange(
        spreading_source, helmholtz_inverses, heat_spreading_coupler
    )
    heat_updated = (heat_source.astype(jnp.float32) - coupled_out.astype(jnp.float32)).astype(
        jnp.bfloat16
    )
    level_gain = lax.dynamic_slice_in_dim(smoothing_strengths, lev_index * lev_local, lev_local)
    damping = damping_table(level_gain, jnp.arange(total_n, dtype=jnp.int32), total_n)
    spin_updated = (spin_tendency.astype(jnp.float32) * damping[None, None]).astype(jnp.bfloat16)
    interior_slice = (
        jnp.arange(total_n, dtype=jnp.int32)[None, :] >= azimuthal_order_list[:, None]
    )[:, None, None, :]
    return (
        jnp.where(interior_slice, spin_updated, empty_placeholder),
        jnp.where(interior_slice, spreading_updated, empty_placeholder),
        jnp.where(interior_slice, heat_updated, empty_placeholder),
    )


def solution(mesh):
    return jax.shard_map(
        on_device,
        mesh=mesh,
        in_specs=(
            P("wave", None, "lev", None),
            P("wave", None, "lev", None),
            P("wave", None, "lev", None),
            P("lev", "wave", None, None),
            P(),
            P(),
            P("wave"),
        ),
        out_specs=(
            P("wave", None, "lev", None),
            P("wave", None, "lev", None),
            P("wave", None, "lev", None),
        ),
        check_vma=False,
    )
```
